32 devices in a mesh: seq: 16 (over z, y, x), blk: 2 (over core).
Axes of the slice: x: 2, y: 2, z: 4, core: 2. Of those that a mesh axis runs over, the one named last changes fastest.
Arguments:
- query: bfloat16 [2048, 5120], P(('blk', 'seq')), may hold values from -139 to 139
- keys: bfloat16 [2048, 5120], P(('blk', 'seq')), may hold values from -4.5 to 4.5
- values: bfloat16 [2048, 5120], P(('blk', 'seq')), may hold values from -6 to 6
Outputs:
- attended: bfloat16 [2048, 5120], P(('blk', 'seq'))
The draws below stay inside these ranges and needn't reach their ends.
All inputs are finite; a program needn't handle non-finite values.
Results may differ from the reference program's by a relative error of at most 0.008.
Values may be sent and summed in bfloat16 or wider, within the bound.
A program may use at most 64 MiB of HBM per device.

```python
import jax
import jax.numpy as jnp
from jax import lax

HEADS = 40
HEAD_DIM = 128
SEQ_LEN = 2048


def joint_draw(key):
    base = jax.random.fold_in(key, 7)
    first, second = jax.random.split(base, 2)
    shape = (SEQ_LEN, HEADS * HEAD_DIM)
    keys = jnp.clip(jax.random.normal(first, shape, jnp.float32), -4.5, 4.5)
    query = jnp.clip(jax.random.normal(second, shape, jnp.float32), -4.5, 4.5)
    return (query, keys)


def draw_query(key, part):
    return joint_draw(key)[0].astype(jnp.bfloat16)


def draw_keys(key, part):
    return joint_draw(key)[1].astype(jnp.bfloat16)


def level_of(own_key, shape, pieces, smallest, top_value):
    level = 1.0
    for axis_at, parts in pieces:
        heights = jax.random.uniform(jax.random.fold_in(jax.random.fold_in(own_key, 6), axis_at), (parts,), jnp.float32, smallest / len(pieces), top_value / len(pieces))
        level = level * jnp.repeat(jnp.exp(heights), shape[axis_at] // parts).reshape((-1,) + (1,) * (len(shape) - 1 - axis_at))
    return level


def scatter_about(rng, extent, scale, reach, cuts=(), held_as=jnp.bfloat16):
    factor_of = level_of(rng, extent, cuts, -0.22, 0.18) if cuts else 1.0
    values = jax.random.normal(rng, extent, jnp.float32) * scale * factor_of
    return jnp.minimum(jnp.maximum(values, -reach), reach).astype(held_as)


def setup_inputs(seed: int = 0) -> dict:
    splits = jax.random.split(jax.random.key(seed), 4)
    return {
        "query": draw_query(jax.random.fold_in(splits[3], 71), 0),
        "keys": draw_keys(jax.random.fold_in(splits[3], 71), 0),
        "values": scatter_about(splits[2], (SEQ_LEN, HEADS * HEAD_DIM), 1.0, 6.0, ((0, 32),)),
    }


def reference(query, keys, values):
    length = query.shape[0]
    width = HEAD_DIM
    rows = min(512, length)

    def heads_first(array):
        return jnp.transpose(array.reshape(length, HEADS, width), (1, 0, 2))

    def one_head(args):
        q_head, k_head, v_head = args

        def block(q_rows):
            scores = lax.dot_general(q_rows, k_head, (((1,), (1,)), ((), ())), preferred_element_type=jnp.float32) * (width ** -0.5)
            peak = jnp.max(scores, axis=1, keepdims=True)
            expo = jnp.exp(scores - peak)
            totals = jnp.sum(expo, axis=1)
            summed = jnp.dot(expo.astype(jnp.bfloat16), v_head, preferred_element_type=jnp.float32)
            return (summed / totals[:, None]).astype(jnp.bfloat16)

        return lax.map(block, q_head.reshape(length // rows, rows, width)).reshape(length, width)

    result = lax.map(one_head, (heads_first(query), heads_first(keys), heads_first(values)))
    return jnp.transpose(result, (1, 0, 2)).reshape(length, HEADS * width)
```

```python
import functools
import math

import jax
import jax.numpy as jnp
from jax import lax
from jax.experimental import pallas as pl
from jax.experimental.pallas import tpu as pltpu
from jax.sharding import PartitionSpec as P

HEADS = 40
MESH = pl.DeviceIdType.MESH


def waves(groups):
    pivot = 2 if groups > 2 else 0
    half = groups // 2
    order = sorted(range(1, groups), key=lambda o: (o < half, not o & pivot, o))
    first = []
    for offset in order:
        if offset == pivot or offset ^ pivot not in first:
            first.append(offset)
    return pivot, first, [offset for offset in order if offset not in first]


def kernel(
    groups, ranks, cores, per_group, width,
    q_hbm, k_hbm, v_hbm, out,
    q_in, k_in, v_in, q_buf, k_buf, v_buf, o_buf,
    load_sem, send_sem, fwd_sem, o_send, q_sem, k_sem, v_sem, o_sem, ready_sem,
):
    tok = q_in.shape[0]
    me = lax.axis_index("seq")
    blk = lax.axis_index("blk")
    group = me // ranks
    rank = lax.rem(me, ranks)
    half = max(groups // 2, 1)
    pivot, first, second = waves(groups)
    mine = rank * cores + blk
    scale = width ** (-0.5) * math.log2(math.e)

    loads = [
        pltpu.make_async_copy(source, kept, load_sem.at[index])
        for index, (source, kept) in enumerate(
            ((k_hbm, k_in), (v_hbm, v_in), (q_hbm, q_in))
        )
    ]
    for load in loads:
        load.start()

    barrier = pltpu.get_barrier_semaphore()
    peers = [{"seq": (group ^ offset) * ranks + rank} for offset in first]
    peers += [
        {"seq": group * ranks + lax.rem(rank + step, ranks)} for step in range(1, ranks)
    ]
    peers += [{"blk": lax.rem(blk + step, cores)} for step in range(1, cores)]
    for peer in peers:
        pl.semaphore_signal(barrier, inc=1, device_id=peer, device_id_type=MESH)
    pl.semaphore_wait(barrier, len(peers))
    if second:
        pl.semaphore_signal(
            ready_sem, inc=1, device_id=peers[first.index(pivot)], device_id_type=MESH
        )

    def columns(g, h):
        return pl.ds(pl.multiple_of((g * per_group + h) * width, width), width)

    def rows(g):
        return pl.ds(pl.multiple_of(g * tok, tok), tok)

    def spread(h, source, landing, index, recv, offsets):
        for offset in offsets:
            other = group ^ offset
            pltpu.make_async_remote_copy(
                src_ref=source.at[:, columns(other, h)],
                dst_ref=landing.at[index + (rows(group),)],
                send_sem=send_sem.at[h],
                recv_sem=recv,
                device_id={"seq": other * ranks + rank},
                device_id_type=MESH,
            ).start()

    def keep(h, source, landing, index, recv):
        pltpu.make_async_copy(
            source.at[:, columns(group, h)], landing.at[index + (rows(group),)], recv
        ).start()

    def issue_kv(h, offsets, own):
        for source, buf, sem in ((k_in, k_buf, k_sem), (v_in, v_buf, v_sem)):
            spread(h, source, buf, (h, mine), sem.at[h, mine], offsets)
            if own:
                keep(h, source, buf, (h, mine), sem.at[h, mine])

    def issue_q(h):
        spread(h, q_in, q_buf, (h,), q_sem.at[h], first + second)
        keep(h, q_in, q_buf, (h,), q_sem.at[h])

    def arrived(buf, sem):
        pltpu.make_async_copy(buf, buf, sem).wait()

    def forward(h, buf, sem, part, target):
        pltpu.make_async_remote_copy(
            src_ref=buf.at[h, part],
            dst_ref=buf.at[h, part],
            send_sem=fwd_sem.at[h],
            recv_sem=sem.at[h, part],
            device_id=target,
            device_id_type=MESH,
        ).start()

    def to_cores(h, buf, sem, part):
        for step in range(1, cores):
            forward(h, buf, sem, part, {"blk": lax.rem(blk + step, cores)})

    def to_ranks(h, buf, sem, part):
        for step in range(1, ranks):
            peer = group * ranks + lax.rem(rank + step, ranks)
            forward(h, buf, sem, part, {"seq": peer})

    def update(h, part, state):
        scores = lax.dot_general(
            q_buf[h], k_buf[h, part], (((1,), (1,)), ((), ())),
            preferred_element_type=jnp.float32,
        )
        peak = jnp.max(scores, axis=1, keepdims=True)
        if state is not None:
            peak = jnp.maximum(peak, state[0])
        expo = jnp.exp2((scores - peak) * scale)
        total = jnp.sum(expo, axis=1, keepdims=True)
        summed = jnp.dot(
            expo.astype(jnp.bfloat16), v_buf[h, part], preferred_element_type=jnp.float32
        )
        if state is not None:
            fade = jnp.exp2((state[0] - peak) * scale)
            total += fade * state[1]
            summed += fade * state[2]
        return (peak, total, summed)

    def near(h):
        for buf, sem in ((k_buf, k_sem), (v_buf, v_sem)):
            arrived(buf.at[h, mine], sem.at[h, mine])
            to_ranks(h, buf, sem, mine)
            to_cores(h, buf, sem, mine)

    def far(h):
        for hop in range(1, ranks):
            part = lax.rem(rank + hop, ranks) * cores + blk
            for buf, sem in ((k_buf, k_sem), (v_buf, v_sem)):
                arrived(buf.at[h, part], sem.at[h, part])
                to_cores(h, buf, sem, part)

    def attend(h):
        arrived(q_buf.at[h], q_sem.at[h])
        parts = [
            lax.rem(rank + hop, ranks) * cores + lax.rem(blk + step, cores)
            for step in range(cores)
            for hop in range(ranks)
        ]
        for part in parts[ranks:]:
            arrived(k_buf.at[h, part], k_sem.at[h, part])
            arrived(v_buf.at[h, part], v_sem.at[h, part])
        state = None
        for part in parts:
            state = update(h, part, state)
        o_buf[h] = (state[2] / state[1]).astype(o_buf.dtype)

    def give(h):
        away = (1 - group // half) * half
        targets = [away + i for i in range(half)] if groups > 1 else []
        targets += [group ^ offset for offset in range(1, half)]
        for other in targets:
            pltpu.make_async_remote_copy(
                src_ref=o_buf.at[h, rows(other)],
                dst_ref=out.at[:, columns(group, h)],
                send_sem=o_send.at[h],
                recv_sem=o_sem.at[h],
                device_id={"seq": other * ranks + rank},
                device_id_type=MESH,
            ).start()
        pltpu.make_async_copy(
            o_buf.at[h, rows(group)], out.at[:, columns(group, h)], o_sem.at[h]
        ).start()

    last = per_group - 1

    loads[0].wait()
    loads[1].wait()
    early = [offset for offset in first if offset >= half]
    late = [offset for offset in first if offset < half] + second
    inner = (group >= groups // 4) & (group < groups - groups // 4)

    issue_kv(0, first, True)
    if second:
        if per_group > 1:

            @pl.when(inner)
            def _():
                issue_kv(1, early, False)

        pl.semaphore_wait(ready_sem, 1)
        issue_kv(0, second, False)
        if per_group > 1:

            @pl.when(jnp.logical_not(inner))
            def _():
                issue_kv(1, early, False)

    elif per_group > 1:
        issue_kv(1, early, False)
    if per_group > 1:
        issue_kv(1, late, True)
    loads[2].wait()
    near(0)

    def queries(start, stop):
        def one(h, _):
            issue_q(h)
            return 0

        lax.fori_loop(start, stop, one, 0)

    lag = max(last - 1, 0)
    some = min(2, per_group)

    def step(s, _):
        @pl.when(s + 2 <= last)
        def _():
            issue_kv(s + 2, first + second, True)

        @pl.when(s == lag)
        def _():
            queries(0, some)

        @pl.when(s + 1 <= last)
        def _():
            near(s + 1)

        @pl.when(s == lag)
        def _():
            queries(some, per_group)

        @pl.when(s <= last)
        def _():
            far(s)

        @pl.when(s >= lag)
        def _():
            attend(s - lag)
            give(s - lag)

        return 0

    lax.fori_loop(0, per_group + lag, step, 0)

    away = pl.ds(0, (groups - 1) * tok)

    def finish(h, _):
        for _ in range(3):
            arrived(q_buf.at[h, away], send_sem.at[h])
        arrived(q_buf.at[h, away], o_send.at[h])
        count = 2 * (ranks - 1 + ranks * (cores - 1))
        for _ in range(count):
            arrived(q_buf.at[h], fwd_sem.at[h])
        arrived(o_buf.at[h], o_sem.at[h])
        return 0

    lax.fori_loop(0, per_group, finish, 0)


def place(source, out, sem):
    copy = pltpu.make_async_copy(source, out, sem)
    copy.start()
    copy.wait()


def on_device(query, keys, values):
    seq = lax.axis_size("seq")
    cores = lax.axis_size("blk")
    tok, columns = query.shape
    width = columns // HEADS
    groups = math.gcd(seq, HEADS)
    ranks = seq // groups
    per_group = HEADS // groups
    parts = ranks * cores
    span = groups * tok
    dtype = query.dtype
    vmem = pl.BlockSpec(memory_space=pltpu.VMEM)
    dma = pltpu.SemaphoreType.DMA
    held = (2 * parts + 2) * per_group * span * width * dtype.itemsize
    inputs = [
        pltpu.with_memory_space_constraint(array, pltpu.HBM)
        for array in (query, keys, values)
    ]
    landed = pl.pallas_call(
        functools.partial(kernel, groups, ranks, cores, per_group, width),
        out_shape=pltpu.VMEM(query.shape, dtype),
        in_specs=[pl.BlockSpec(memory_space=pl.ANY)] * 3,
        out_specs=vmem,
        scratch_shapes=[
            pltpu.VMEM(query.shape, dtype),
            pltpu.VMEM(query.shape, dtype),
            pltpu.VMEM(query.shape, dtype),
            pltpu.VMEM((per_group, span, width), dtype),
            pltpu.VMEM((per_group, parts, span, width), dtype),
            pltpu.VMEM((per_group, parts, span, width), dtype),
            pltpu.VMEM((per_group, span, width), dtype),
            dma((3,)),
            dma((per_group,)),
            dma((per_group,)),
            dma((per_group,)),
            dma((per_group,)),
            dma((per_group, parts)),
            dma((per_group, parts)),
            dma((per_group,)),
            pltpu.SemaphoreType.REGULAR,
        ],
        compiler_params=pltpu.CompilerParams(
            collective_id=0,
            has_side_effects=True,
            vmem_limit_bytes=held + 20 * 1024 * 1024,
        ),
    )(*inputs)
    return pl.pallas_call(
        place,
        out_shape=jax.ShapeDtypeStruct(query.shape, dtype),
        in_specs=[vmem],
        out_specs=pl.BlockSpec(memory_space=pl.ANY),
        scratch_shapes=[dma],
        compiler_params=pltpu.CompilerParams(vmem_limit_bytes=4 * 1024 * 1024),
    )(landed)


def solution(mesh):
    spec = P(("blk", "seq"), None)
    return jax.shard_map(
        on_device, mesh=mesh, in_specs=(spec,) * 3, out_specs=spec, check_vma=False
    )
```

```python
import functools
import math

import jax
import jax.numpy as jnp
from jax import lax
from jax.experimental import pallas as pl
from jax.experimental.pallas import tpu as pltpu
from jax.sharding import PartitionSpec as P

HEADS = 40
MESH = pl.DeviceIdType.MESH


def kernel(
    groups, ranks, cores, per_group, width,
    q_hbm, k_hbm, v_hbm, out,
    q_in, k_in, v_in, q_buf, k_buf, v_buf, o_buf,
    load_sem, send_sem, fwd_sem, o_send, q_sem, k_sem, v_sem, o_sem, ready_sem,
):
    tok = q_in.shape[0]
    me = lax.axis_index("seq")
    blk = lax.axis_index("blk")
    group = me // ranks
    rank = lax.rem(me, ranks)
    half = max(groups // 2, 1)
    staged = groups >= 4
    quarter = groups // 4 if staged else 0
    mirror = groups - quarter
    rest = [offset for offset in range(half, groups) if offset != mirror]
    rest = sorted(rest, key=lambda offset: -(offset > mirror)) + list(range(half - 1, 0, -1))
    inner = (group >= quarter) & (group < groups - quarter) if staged else None
    mine = rank * cores + blk
    scale = width ** (-0.5) * math.log2(math.e)

    loads = [
        pltpu.make_async_copy(source, kept, load_sem.at[index])
        for index, (source, kept) in enumerate(
            ((k_hbm, k_in), (v_hbm, v_in), (q_hbm, q_in))
        )
    ]
    loads[0].start()
    loads[1].start()

    barrier = pltpu.get_barrier_semaphore()

    def at(offset):
        return {"seq": (group ^ offset) * ranks + rank}

    def other_rank(step):
        return {"seq": group * ranks + lax.rem(rank + step, ranks)}

    def other_core(step):
        return {"blk": lax.rem(blk + step, cores)}

    def tell(sem, peer):
        pl.semaphore_signal(sem, inc=1, device_id=peer, device_id_type=MESH)

    def tell_if(condition, sem, peer):
        @pl.when(condition)
        def _():
            tell(sem, peer)

    total = groups - 1 + ranks - 1 + cores - 1
    if staged:
        outer = jnp.logical_not(inner)
        tell(barrier, at(mirror))
        for offset in rest:
            across = offset < quarter or offset > mirror
            tell_if(outer if across else inner, barrier, at(offset))
        for step in range(1, ranks):
            tell_if(outer | (rank + step < ranks), barrier, other_rank(step))
        for step in range(1, cores):
            tell_if(outer | (blk + step < cores), barrier, other_core(step))
        pl.semaphore_wait(barrier, jnp.where(inner, 1 + rank + blk, total))
        tell_if(outer, ready_sem, at(quarter))
        for step in range(1, ranks):
            tell_if(inner & (rank + step >= ranks), ready_sem, other_rank(step))
        for step in range(1, cores):
            tell_if(inner & (blk + step >= cores), ready_sem, other_core(step))
    else:
        for offset in range(1, groups):
            tell(barrier, at(offset))
        for step in range(1, ranks):
            tell(barrier, other_rank(step))
        for step in range(1, cores):
            tell(barrier, other_core(step))
        pl.semaphore_wait(barrier, total)

    def columns(g, h):
        return pl.ds(pl.multiple_of((g * per_group + h) * width, width), width)

    def rows(g):
        return pl.ds(pl.multiple_of(g * tok, tok), tok)

    def spread(h, source, landing, index, recv, offsets):
        for offset in offsets:
            other = group ^ offset
            pltpu.make_async_remote_copy(
                src_ref=source.at[:, columns(other, h)],
                dst_ref=landing.at[index + (rows(group),)],
                send_sem=send_sem.at[h],
                recv_sem=recv,
                device_id={"seq": other * ranks + rank},
                device_id_type=MESH,
            ).start()

    def keep(h, source, landing, index, recv):
        pltpu.make_async_copy(
            source.at[:, columns(group, h)], landing.at[index + (rows(group),)], recv
        ).start()

    every = ([mirror] if staged else []) + rest

    def issue_kv(h, offsets, own):
        for source, buf, sem in ((k_in, k_buf, k_sem), (v_in, v_buf, v_sem)):
            spread(h, source, buf, (h, mine), sem.at[h, mine], offsets)
            if own:
                keep(h, source, buf, (h, mine), sem.at[h, mine])

    def issue_q(h):
        spread(h, q_in, q_buf, (h,), q_sem.at[h], every)
        keep(h, q_in, q_buf, (h,), q_sem.at[h])

    def arrived(buf, sem):
        pltpu.make_async_copy(buf, buf, sem).wait()

    def forward(h, buf, sem, part, target):
        pltpu.make_async_remote_copy(
            src_ref=buf.at[h, part],
            dst_ref=buf.at[h, part],
            send_sem=fwd_sem.at[h],
            recv_sem=sem.at[h, part],
            device_id=target,
            device_id_type=MESH,
        ).start()

    def to_cores(h, buf, sem, part):
        for step in range(1, cores):
            forward(h, buf, sem, part, {"blk": lax.rem(blk + step, cores)})

    def to_ranks(h, buf, sem, part):
        for step in range(1, ranks):
            peer = group * ranks + lax.rem(rank + step, ranks)
            forward(h, buf, sem, part, {"seq": peer})

    def update(h, part, state):
        scores = lax.dot_general(
            q_buf[h], k_buf[h, part], (((1,), (1,)), ((), ())),
            preferred_element_type=jnp.float32,
        )
        peak = jnp.max(scores, axis=1, keepdims=True)
        if state is not None:
            peak = jnp.maximum(peak, state[0])
        expo = jnp.exp2((scores - peak) * scale)
        total = jnp.sum(expo, axis=1, keepdims=True)
        summed = jnp.dot(
            expo.astype(jnp.bfloat16), v_buf[h, part], preferred_element_type=jnp.float32
        )
        if state is not None:
            fade = jnp.exp2((state[0] - peak) * scale)
            total += fade * state[1]
            summed += fade * state[2]
        return (peak, total, summed)

    def near(h):
        for buf, sem in ((k_buf, k_sem), (v_buf, v_sem)):
            arrived(buf.at[h, mine], sem.at[h, mine])
            to_ranks(h, buf, sem, mine)
            to_cores(h, buf, sem, mine)

    def far(h):
        for hop in range(1, ranks):
            part = lax.rem(rank + hop, ranks) * cores + blk
            for buf, sem in ((k_buf, k_sem), (v_buf, v_sem)):
                arrived(buf.at[h, part], sem.at[h, part])
                to_cores(h, buf, sem, part)

    def attend(h):
        arrived(q_buf.at[h], q_sem.at[h])
        parts = [
            lax.rem(rank + hop, ranks) * cores + lax.rem(blk + step, cores)
            for step in range(cores)
            for hop in range(ranks)
        ]
        for part in parts[ranks:]:
            arrived(k_buf.at[h, part], k_sem.at[h, part])
            arrived(v_buf.at[h, part], v_sem.at[h, part])
        state = None
        for part in parts:
            state = update(h, part, state)
        o_buf[h] = (state[2] / state[1]).astype(o_buf.dtype)

    def send_out(h, other):
        pltpu.make_async_remote_copy(
            src_ref=o_buf.at[h, rows(other)],
            dst_ref=out.at[:, columns(group, h)],
            send_sem=o_send.at[h],
            recv_sem=o_sem.at[h],
            device_id={"seq": other * ranks + rank},
            device_id_type=MESH,
        ).start()

    def give_first(h):
        @pl.when(group != 0)
        def _():
            send_out(h, 0)

    def give_rest(h):
        away = (1 - group // half) * half
        targets = [away + i for i in range(half)] if groups > 1 else []
        targets += [group ^ offset for offset in range(half - 1, 0, -1)]
        for other in targets:

            @pl.when(other != 0)
            def _():
                send_out(h, other)

        pltpu.make_async_copy(
            o_buf.at[h, rows(group)], out.at[:, columns(group, h)], o_sem.at[h]
        ).start()

    def hand_out(h):
        held = max(last - 1, 0)
        early = max(last - 2, 0)
        upper = group >= half

        def rest_of(start, stop):
            def one(i, _):
                give_rest(i)
                return 0

            lax.fori_loop(start, stop, one, 0)

        give_first(h)
        if not staged:
            give_rest(h)
            return

        @pl.when(inner & jnp.logical_not(upper))
        def _():
            give_rest(h)

        @pl.when(outer & (h == jnp.where(upper, early - 1, held)))
        def _():
            rest_of(0, h + 1)

        @pl.when((h == last) & (outer | upper))
        def _():
            rest_of(jnp.where(upper, jnp.where(inner, 0, early), held + 1), per_group)

    loads[0].wait()
    loads[1].wait()
    loads[2].start()

    def to_mirror(h, _):
        issue_kv(h, [mirror], False)
        return 0

    def to_rest(h, _):
        issue_kv(h, rest, True)
        return 0

    def to_all(h, _):
        issue_kv(h, every, True)
        return 0

    def queries(h, _):
        issue_q(h)
        return 0

    def ask():
        loads[2].wait()
        lax.fori_loop(0, per_group, queries, 0)

    last = per_group - 1
    lag = max(last - 1, 1)

    if staged:

        @pl.when(inner)
        def _():
            lax.fori_loop(0, per_group, to_mirror, 0)
            waited = 1 + ranks - 1 - rank + cores - 1 - blk
            pl.semaphore_wait(ready_sem, waited)
            lax.fori_loop(0, per_group, to_rest, 0)
            ask()

        @pl.when(outer)
        def _():
            to_all(0, 0)

    else:
        lax.fori_loop(0, per_group, to_all, 0)
        ask()

    def collect(h):
        near(h)
        if staged:

            @pl.when(outer & (h < last))
            def _():
                to_all(h + 1, 0)

            @pl.when(outer & (h == max(last - 1, 0)))
            def _():
                ask()

    collect(0)

    def step(s, _):
        @pl.when(s + 1 <= last)
        def _():
            collect(s + 1)

        @pl.when((s >= 1) & (s <= last + 1))
        def _():
            far(s - 1)

        @pl.when(s >= lag)
        def _():
            attend(s - lag)
            hand_out(s - lag)

        return 0

    lax.fori_loop(0, per_group + lag, step, 0)

    away = pl.ds(0, (groups - 1) * tok)

    def finish(h, _):
        for _ in range(3):
            arrived(q_buf.at[h, away], send_sem.at[h])
        arrived(q_buf.at[h, away], o_send.at[h])
        count = 2 * (ranks - 1 + ranks * (cores - 1))
        for _ in range(count):
            arrived(q_buf.at[h], fwd_sem.at[h])
        arrived(o_buf.at[h], o_sem.at[h])
        return 0

    lax.fori_loop(0, per_group, finish, 0)


def place(source, out, sem):
    copy = pltpu.make_async_copy(source, out, sem)
    copy.start()
    copy.wait()


def on_device(query, keys, values):
    seq = lax.axis_size("seq")
    cores = lax.axis_size("blk")
    tok, columns = query.shape
    width = columns // HEADS
    groups = math.gcd(seq, HEADS)
    ranks = seq // groups
    per_group = HEADS // groups
    parts = ranks * cores
    span = groups * tok
    dtype = query.dtype
    vmem = pl.BlockSpec(memory_space=pltpu.VMEM)
    dma = pltpu.SemaphoreType.DMA
    held = (2 * parts + 2) * per_group * span * width * dtype.itemsize
    inputs = [
        pltpu.with_memory_space_constraint(array, pltpu.HBM)
        for array in (query, keys, values)
    ]
    landed = pl.pallas_call(
        functools.partial(kernel, groups, ranks, cores, per_group, width),
        out_shape=pltpu.VMEM(query.shape, dtype),
        in_specs=[pl.BlockSpec(memory_space=pl.ANY)] * 3,
        out_specs=vmem,
        scratch_shapes=[
            pltpu.VMEM(query.shape, dtype),
            pltpu.VMEM(query.shape, dtype),
            pltpu.VMEM(query.shape, dtype),
            pltpu.VMEM((per_group, span, width), dtype),
            pltpu.VMEM((per_group, parts, span, width), dtype),
            pltpu.VMEM((per_group, parts, span, width), dtype),
            pltpu.VMEM((per_group, span, width), dtype),
            dma((3,)),
            dma((per_group,)),
            dma((per_group,)),
            dma((per_group,)),
            dma((per_group,)),
            dma((per_group, parts)),
            dma((per_group, parts)),
            dma((per_group,)),
            pltpu.SemaphoreType.REGULAR,
        ],
        compiler_params=pltpu.CompilerParams(
            collective_id=0,
            has_side_effects=True,
            vmem_limit_bytes=held + 20 * 1024 * 1024,
        ),
    )(*inputs)
    return pl.pallas_call(
        place,
        out_shape=jax.ShapeDtypeStruct(query.shape, dtype),
        in_specs=[vmem],
        out_specs=pl.BlockSpec(memory_space=pl.ANY),
        scratch_shapes=[dma],
        compiler_params=pltpu.CompilerParams(vmem_limit_bytes=4 * 1024 * 1024),
    )(landed)


def solution(mesh):
    spec = P(("blk", "seq"), None)
    return jax.shard_map(
        on_device, mesh=mesh, in_specs=(spec,) * 3, out_specs=spec, check_vma=False
    )
```

```python
import functools
import math

import jax
import jax.numpy as jnp
from jax import lax
from jax.experimental import pallas as pl
from jax.experimental.pallas import tpu as pltpu
from jax.sharding import PartitionSpec as P

HEADS = 40
MESH = pl.DeviceIdType.MESH


def kernel(
    groups, ranks, cores, per_group, width,
    q_hbm, k_hbm, v_hbm, out,
    q_in, k_in, v_in, q_buf, kv_buf, o_buf,
    load_sem, send_sem, near_sem, far_sem, rest_sem, o_sem, ready_sem,
):
    tok = q_in.shape[0]
    me = lax.axis_index("seq")
    blk = lax.axis_index("blk")
    group = me // ranks
    rank = lax.rem(me, ranks)
    half = max(groups // 2, 1)
    staged = groups >= 4
    quarter = groups // 4 if staged else 0
    mirror = groups - quarter
    rest = [offset for offset in range(half, groups) if offset != mirror]
    rest = sorted(rest, key=lambda offset: -(offset > mirror)) + list(range(half - 1, 0, -1))
    inner = (group >= quarter) & (group < groups - quarter) if staged else None
    mine = rank * cores + blk
    scale = width ** (-0.5) * math.log2(math.e)

    span = per_group * width
    sources = ((k_hbm, k_in), (v_hbm, v_in), (q_hbm, q_in))

    def fetch(index, offsets, sem):
        source, kept = sources[index]
        for offset in offsets:
            first = pl.multiple_of((group ^ offset) * span, span)
            block = (slice(None), pl.ds(first, span))
            pltpu.make_async_copy(source.at[block], kept.at[block], sem).start()

    def fetched(count, sem):
        kept = q_in.at[:, pl.ds(0, count * span)]
        pltpu.make_async_copy(kept, kept, sem).wait()

    early_load = [mirror] if staged else []
    late_load = [offset for offset in range(groups) if offset not in early_load]

    def fetch_late():
        for index in range(2):
            fetch(index, late_load, load_sem.at[1])

    for index in range(2):
        fetch(index, early_load, load_sem.at[0])

    barrier = pltpu.get_barrier_semaphore()

    def at(offset):
        return {"seq": (group ^ offset) * ranks + rank}

    def other_rank(step):
        return {"seq": group * ranks + lax.rem(rank + step, ranks)}

    def other_core(step):
        return {"blk": lax.rem(blk + step, cores)}

    def tell(sem, peer):
        pl.semaphore_signal(sem, inc=1, device_id=peer, device_id_type=MESH)

    def tell_if(condition, sem, peer):
        @pl.when(condition)
        def _():
            tell(sem, peer)

    total = groups - 1 + ranks - 1 + cores - 1
    if staged:
        outer = jnp.logical_not(inner)
        tell(barrier, at(mirror))
        for offset in rest:
            across = offset < quarter or offset > mirror
            tell_if(outer if across else inner, barrier, at(offset))
        for step in range(1, ranks):
            tell_if(outer | (rank + step < ranks), barrier, other_rank(step))
        for step in range(1, cores):
            tell_if(outer | (blk + step < cores), barrier, other_core(step))
        fetch_late()
        pl.semaphore_wait(barrier, jnp.where(inner, 1 + rank + blk, total))
        tell_if(outer, ready_sem, at(quarter))
        for step in range(1, ranks):
            tell_if(inner & (rank + step >= ranks), ready_sem, other_rank(step))
        for step in range(1, cores):
            tell_if(inner & (blk + step >= cores), ready_sem, other_core(step))
    else:
        for offset in range(1, groups):
            tell(barrier, at(offset))
        for step in range(1, ranks):
            tell(barrier, other_rank(step))
        for step in range(1, cores):
            tell(barrier, other_core(step))
        fetch_late()
        pl.semaphore_wait(barrier, total)

    def columns(g, h):
        return pl.ds(pl.multiple_of((g * per_group + h) * width, width), width)

    def rows(g):
        return pl.ds(pl.multiple_of(g * tok, tok), tok)

    def spread(h, source, landing, index, recv, offsets):
        for offset in offsets:
            other = group ^ offset
            pltpu.make_async_remote_copy(
                src_ref=source.at[:, columns(other, h)],
                dst_ref=landing.at[index + (rows(group),)],
                send_sem=send_sem,
                recv_sem=recv,
                device_id={"seq": other * ranks + rank},
                device_id_type=MESH,
            ).start()

    def keep(h, source, landing, index, recv):
        pltpu.make_async_copy(
            source.at[:, columns(group, h)], landing.at[index + (rows(group),)], recv
        ).start()

    every = ([mirror] if staged else []) + rest

    def issue_kv(h, offsets, own):
        for index, source in enumerate((k_in, v_in)):
            slot = (h, 2 * mine + index)
            spread(h, source, kv_buf, slot, near_sem.at[h], offsets)
            if own:
                keep(h, source, kv_buf, slot, near_sem.at[h])

    def issue_q(h):
        spread(h, q_in, q_buf, (h,), rest_sem.at[h], every)
        keep(h, q_in, q_buf, (h,), rest_sem.at[h])

    def arrived(buf, sem):
        pltpu.make_async_copy(buf, buf, sem).wait()

    def pair(h, part):
        return kv_buf.at[h, pl.ds(2 * part, 2)]

    def forward(h, part, sem, target):
        pltpu.make_async_remote_copy(
            src_ref=pair(h, part),
            dst_ref=pair(h, part),
            send_sem=send_sem,
            recv_sem=sem.at[h],
            device_id=target,
            device_id_type=MESH,
        ).start()

    def to_cores(h, part):
        for step in range(1, cores):
            forward(h, part, rest_sem, other_core(step))

    def to_ranks(h):
        for step in range(1, ranks):
            forward(h, mine, far_sem, other_rank(step))

    def update(h, part, state):
        scores = lax.dot_general(
            q_buf[h], kv_buf[h, 2 * part], (((1,), (1,)), ((), ())),
            preferred_element_type=jnp.float32,
        )
        peak = jnp.max(scores, axis=1, keepdims=True)
        if state is not None:
            peak = jnp.maximum(peak, state[0])
        expo = jnp.exp2((scores - peak) * scale)
        total = jnp.sum(expo, axis=1, keepdims=True)
        summed = jnp.dot(
            expo.astype(jnp.bfloat16), kv_buf[h, 2 * part + 1],
            preferred_element_type=jnp.float32,
        )
        if state is not None:
            fade = jnp.exp2((state[0] - peak) * scale)
            total += fade * state[1]
            summed += fade * state[2]
        return (peak, total, summed)

    def near(h):
        arrived(pair(h, mine), near_sem.at[h])
        to_ranks(h)
        to_cores(h, mine)

    def far(h):
        if ranks > 1:
            arrived(kv_buf.at[h, pl.ds(0, 2 * (ranks - 1))], far_sem.at[h])
        for hop in range(1, ranks):
            to_cores(h, lax.rem(rank + hop, ranks) * cores + blk)

    def attend(h):
        blocks = 2 * ranks * (cores - 1) + 1
        arrived(kv_buf.at[h, pl.ds(0, blocks)], rest_sem.at[h])
        parts = [
            lax.rem(rank + hop, ranks) * cores + lax.rem(blk + step, cores)
            for step in range(cores)
            for hop in range(ranks)
        ]
        state = None
        for part in parts:
            state = update(h, part, state)
        o_buf[h] = (state[2] / state[1]).astype(o_buf.dtype)

    def send_out(h, other):
        pltpu.make_async_remote_copy(
            src_ref=o_buf.at[h, rows(other)],
            dst_ref=out.at[:, columns(group, h)],
            send_sem=send_sem,
            recv_sem=o_sem,
            device_id={"seq": other * ranks + rank},
            device_id_type=MESH,
        ).start()

    def give_first(h):
        @pl.when(group != 0)
        def _():
            send_out(h, 0)

    def give_rest(h):
        away = (1 - group // half) * half
        targets = [away + i for i in range(half)] if groups > 1 else []
        targets += [group ^ offset for offset in range(half - 1, 0, -1)]
        for other in targets:

            @pl.when(other != 0)
            def _():
                send_out(h, other)

        pltpu.make_async_copy(
            o_buf.at[h, rows(group)], out.at[:, columns(group, h)], o_sem
        ).start()

    def hand_out(h):
        held = max(last - 1, 0)
        early = max(last - 2, 0)
        upper = group >= half

        def rest_of(start, stop):
            def one(i, _):
                give_rest(i)
                return 0

            lax.fori_loop(start, stop, one, 0)

        give_first(h)
        if not staged:
            give_rest(h)
            return

        @pl.when(inner & ((h == 0) | jnp.logical_not(upper)))
        def _():
            give_rest(h)

        @pl.when(outer & (h == jnp.where(upper, early - 1, held)))
        def _():
            rest_of(0, h + 1)

        @pl.when((h == last) & (outer | upper))
        def _():
            rest_of(jnp.where(upper, jnp.where(inner, 1, early), held + 1), per_group)

    def to_mirror(h, _):
        issue_kv(h, [mirror], False)
        return 0

    def to_rest(h, _):
        issue_kv(h, rest, True)
        return 0

    def to_all(h, _):
        issue_kv(h, every, True)
        return 0

    def queries(h, _):
        issue_q(h)
        return 0

    def ask():
        fetched(groups, load_sem.at[2])
        lax.fori_loop(0, per_group, queries, 0)

    last = per_group - 1
    lag = max(last - 1, 1)

    if staged:

        @pl.when(inner)
        def _():
            fetched(2, load_sem.at[0])
            lax.fori_loop(0, per_group, to_mirror, 0)
            fetched(groups - 1, load_sem.at[1])
            fetched(groups - 1, load_sem.at[1])
            fetch(2, range(groups), load_sem.at[2])
            waited = 1 + ranks - 1 - rank + cores - 1 - blk
            pl.semaphore_wait(ready_sem, waited)
            lax.fori_loop(0, per_group, to_rest, 0)
            ask()

        @pl.when(outer)
        def _():
            fetched(2, load_sem.at[0])
            fetched(groups - 1, load_sem.at[1])
            fetched(groups - 1, load_sem.at[1])
            fetch(2, range(groups), load_sem.at[2])
            to_all(0, 0)

    else:
        fetched(groups, load_sem.at[1])
        fetched(groups, load_sem.at[1])
        fetch(2, range(groups), load_sem.at[2])
        lax.fori_loop(0, per_group, to_all, 0)
        ask()

    def collect(h):
        near(h)
        if staged:

            @pl.when(outer & (h < last))
            def _():
                to_all(h + 1, 0)

            @pl.when(outer & (h == max(last - 1, 0)))
            def _():
                ask()

    collect(0)

    def step(s, _):
        @pl.when(s + 1 <= last)
        def _():
            collect(s + 1)

        @pl.when((s >= 1) & (s <= last + 1))
        def _():
            far(s - 1)

        @pl.when(s >= lag)
        def _():
            attend(s - lag)
            hand_out(s - lag)

        return 0

    lax.fori_loop(0, per_group + lag, step, 0)

    for _ in range(4):
        arrived(q_buf.at[:, pl.ds(0, (groups - 1) * tok)], send_sem)
    for _ in range(2 * (ranks - 1 + ranks * (cores - 1))):
        arrived(q_buf, send_sem)
    arrived(o_buf, o_sem)


def place(source, out, sem):
    copy = pltpu.make_async_copy(source, out, sem)
    copy.start()
    copy.wait()


def on_device(query, keys, values):
    seq = lax.axis_size("seq")
    cores = lax.axis_size("blk")
    tok, columns = query.shape
    width = columns // HEADS
    groups = math.gcd(seq, HEADS)
    ranks = seq // groups
    per_group = HEADS // groups
    parts = ranks * cores
    span = groups * tok
    dtype = query.dtype
    vmem = pl.BlockSpec(memory_space=pltpu.VMEM)
    dma = pltpu.SemaphoreType.DMA
    held = (2 * parts + 2) * per_group * span * width * dtype.itemsize
    inputs = [
        pltpu.with_memory_space_constraint(array, pltpu.HBM)
        for array in (query, keys, values)
    ]
    landed = pl.pallas_call(
        functools.partial(kernel, groups, ranks, cores, per_group, width),
        out_shape=pltpu.VMEM(query.shape, dtype),
        in_specs=[pl.BlockSpec(memory_space=pl.ANY)] * 3,
        out_specs=vmem,
        scratch_shapes=[
            pltpu.VMEM(query.shape, dtype),
            pltpu.VMEM(query.shape, dtype),
            pltpu.VMEM(query.shape, dtype),
            pltpu.VMEM((per_group, span, width), dtype),
            pltpu.VMEM((per_group, 2 * parts, span, width), dtype),
            pltpu.VMEM((per_group, span, width), dtype),
            dma((3,)),
            dma,
            dma((per_group,)),
            dma((per_group,)),
            dma((per_group,)),
            dma,
            pltpu.SemaphoreType.REGULAR,
        ],
        compiler_params=pltpu.CompilerParams(
            collective_id=0,
            has_side_effects=True,
            vmem_limit_bytes=held + 20 * 1024 * 1024,
        ),
    )(*inputs)
    return pl.pallas_call(
        place,
        out_shape=jax.ShapeDtypeStruct(query.shape, dtype),
        in_specs=[vmem],
        out_specs=pl.BlockSpec(memory_space=pl.ANY),
        scratch_shapes=[dma],
        compiler_params=pltpu.CompilerParams(vmem_limit_bytes=4 * 1024 * 1024),
    )(landed)


def solution(mesh):
    spec = P(("blk", "seq"), None)
    return jax.shard_map(
        on_device, mesh=mesh, in_specs=(spec,) * 3, out_specs=spec, check_vma=False
    )
```
